128 devices in a mesh: group: 8 (over y_lo, z), shard: 16 (over y_hi, x, core).
Axes of the slice: x: 4, y: 4 (y_hi: 2, y_lo: 2; y = y_hi * 2 + y_lo), z: 4, core: 2. Of those that a mesh axis runs over, the one named last changes fastest.
Arguments:
- tokens: bfloat16 [196608, 1024], P(('group', 'shard')), may hold values from -36 to 36
- cotangent: bfloat16 [196608, 1024], P(('group', 'shard')), may hold values from -0.3046875 to 0.3046875
- master: float32 [8192, 4096], P(('group', 'shard')), may hold values from -0.03125 to 0.03125
- moment_one: float32 [8192, 4096], P(('group', 'shard')), may hold values from -2 to 2
- moment_two: float32 [8192, 4096], P(('group', 'shard')), may hold values from 0.05 to 2
- anchor: float32 [1024, 4096], P('shard'), may hold values from -0.03125 to 0.03125
- outer_momentum: float32 [1024, 4096], P('shard'), may hold values from -0.02 to 0.02
Outputs:
- moment_one_next: float32 [8192, 4096], P(('group', 'shard'))
- moment_two_next: float32 [8192, 4096], P(('group', 'shard'))
- momentum_next: float32 [1024, 4096], P('shard')
- anchor_next: float32 [1024, 4096], P('shard')
The draws below stay inside these ranges and needn't reach their ends.
All inputs are finite; a program needn't handle non-finite values.
Results may differ from the reference program's by a relative error of at most 0.0047.
Values may be sent and summed in bfloat16 or wider, within the bound.
A program may use at most 128 MiB of HBM per device.

```python
import math
import jax
import jax.numpy as jnp
from jax import lax

D = 1024
FF = 2048
TOK_DEV = 1536
TOKENS = 196608
ROWS = 8192
N_GROUP = 8
N_SHARD = 16


def steps_of(stream_key, shape, split, smallest, high):
    factor_of, own = 1.0, jax.random.fold_in(stream_key, 6)
    for position, blocks in split:
        steps = jnp.exp(jax.random.uniform(jax.random.fold_in(own, position), (blocks,), jnp.float32, smallest / len(split), high / len(split)))
        factor_of = factor_of * jnp.repeat(steps, shape[position] // blocks).reshape([-1 if axis == position else 1 for axis in range(len(shape))])
    return factor_of


def gaussian(key, dims, spread, limit, shards=(), kind=jnp.bfloat16):
    gain = steps_of(key, dims, shards, -0.22, 0.18) if shards else 1.0
    entries = jax.random.normal(key, dims, jnp.float32) * spread * gain
    return jnp.minimum(jnp.maximum(entries, -limit), limit).astype(kind)


def setup_inputs(seed: int = 0) -> dict:
    seeds = jax.random.split(jax.random.key(seed), 8)
    return {
        "tokens": gaussian(seeds[0], (TOKENS, D), 6.0, 36.0, ((0, 128),)),
        "cotangent": gaussian(seeds[1], (TOKENS, D), (8.0 / (TOK_DEV * N_SHARD) ** 0.5), 0.3046875, ((0, 128),)),
        "master": gaussian(seeds[2], (ROWS, 2 * FF), (36 * D) ** -0.5, 0.03125, ((0, 128),), jnp.float32),
        "moment_one": gaussian(seeds[3], (ROWS, 2 * FF), 0.3, 2.0, ((0, 128),), jnp.float32),
        "moment_two": jnp.clip(jnp.exp(math.log(2.0) - 3.6888794 * jax.random.uniform(seeds[4], (ROWS, 2 * FF), jnp.float32) ** steps_of(seeds[4], (ROWS, 2 * FF), ((0, 128),), -0.2, 0.2)), 0.05, 2.0),
        "anchor": gaussian(seeds[5], (D, 2 * FF), (36 * D) ** -0.5, 0.03125, ((0, 16),), jnp.float32),
        "outer_momentum": gaussian(seeds[6], (D, 2 * FF), 0.0033, 0.02, ((0, 16),), jnp.float32),
    }


first_correction = 0.9999734386011124
second_correction = 0.994079470779664

def gelu_tanh(values):
    return jax.nn.gelu(values, approximate=True)

def reference(tokens, cotangent, master, moment_one, moment_two, anchor, outer_momentum):
    group_rows = TOK_DEV * N_SHARD
    total = jnp.zeros(anchor.shape, jnp.float32)
    first_list = []
    second_list = []
    for group in range(N_GROUP):
        inputs = tokens[group * group_rows:(group + 1) * group_rows]
        upstream = cotangent[group * group_rows:(group + 1) * group_rows]
        params = master[group * D:(group + 1) * D]
        working = params.astype(jnp.bfloat16)
        pre = jnp.dot(inputs, working[:, :FF], preferred_element_type=jnp.float32)
        back = jnp.dot(upstream, working[:, FF:], preferred_element_type=jnp.float32)
        act = gelu_tanh(pre).astype(jnp.bfloat16)
        _, pullback = jax.vjp(gelu_tanh, pre)
        dpre = pullback(back)[0].astype(jnp.bfloat16)
        grad_in = lax.dot_general(inputs, dpre, (((0,), (0,)), ((), ())), preferred_element_type=jnp.float32)
        grad_out = lax.dot_general(upstream, act, (((0,), (0,)), ((), ())), preferred_element_type=jnp.float32)
        grad = jnp.concatenate([grad_in, grad_out], axis=1)
        first = 0.9 * moment_one[group * D:(group + 1) * D] + 0.1 * grad
        second = 0.95 * moment_two[group * D:(group + 1) * D] + 0.05 * grad * grad
        update = first / first_correction / (jnp.sqrt(second / second_correction) + 1e-08)
        inner = params - 0.001 * (update + 0.1 * params)
        total = total + (anchor - inner)
        first_list.append(first)
        second_list.append(second)
    mean_delta = total / N_GROUP
    momentum_next = 0.9 * outer_momentum + mean_delta
    anchor_next = anchor - 0.7 * (mean_delta + 0.9 * momentum_next)
    return (jnp.concatenate(first_list, axis=0), jnp.concatenate(second_list, axis=0), momentum_next, anchor_next)
```

```python
import functools
import jax
import jax.numpy as jnp
from jax import lax
from jax.experimental import pallas as pl
from jax.experimental.pallas import tpu as pltpu
from jax.sharding import PartitionSpec as P

first_correction = 0.9999734386011124
second_correction = 0.994079470779664
MESH = pl.DeviceIdType.MESH
BF = jnp.bfloat16
F32 = jnp.float32
NJ = 4
HB = 256
BT = 512
ROOT = 0.7978845608028654


def gelu_pair(pre, back):
    square = pre * pre
    t = jnp.tanh(pre * (ROOT + (ROOT * 0.044715) * square))
    half = 0.5 + 0.5 * t
    slope = half + pre * (0.5 * ROOT + (1.5 * ROOT * 0.044715) * square) * (1.0 - t * t)
    return pre * half, back * slope


def kernel(
    tok, cot, mas, mo1, mo2, anc, omo,
    o1, o2, om, oa,
    T, C, W, WS, mst, b1, b2, ba, bo, act, dpre, gx, gp, sb, rb, ys, yr, dl, dr, mr,
    loc, tks, tkr, ays, ayr, a1s, a1r, a2s, a2r, rss, rsr, ycs, ycr, m1s, m1r, m2s, m2r, outs,
):
    me = lax.axis_index("group")
    s = lax.axis_index("shard")
    y, x, c = s // 8, (s // 2) % 4, s % 2
    n = lax.axis_size("group")
    td = tok.shape[0]

    def dev(yy, xx, cc):
        return (me, yy * 8 + xx * 2 + cc)

    right = dev(y, lax.rem(x + 1, 4), c)
    left = dev(y, lax.rem(x + 3, 4), c)
    across = (dev(1 - y, x, c), dev(1 - y, x, 1 - c), dev(y, x, 1 - c))

    def send(src, dst, ss, rs, to):
        return pltpu.make_async_remote_copy(
            src_ref=src, dst_ref=dst, send_sem=ss, recv_sem=rs, device_id=to, device_id_type=MESH
        )

    loads = [pltpu.make_async_copy(mas, mst, loc.at[0])]
    for i, (a, b) in enumerate(((mo1, b1), (mo2, b2), (anc, ba), (omo, bo))):
        loads.append(pltpu.make_async_copy(a, b, loc.at[3 + i]))
    loads[0].start()

    def blocks():
        for xx in range(4):
            for yy in range(2):
                yield slice((yy * 4 + xx) * 128, (yy * 4 + xx) * 128 + 128), slice(
                    xx * 256 + yy * 128, xx * 256 + yy * 128 + 128
                )

    for k, (a, b) in enumerate(((tok, T), (cot, C))):
        for cs, cd in blocks():
            pltpu.make_async_copy(a.at[:, cs], b.at[pl.ds(0, td), cd], loc.at[1 + k]).start()

    barrier = pltpu.get_barrier_semaphore()
    for to in (right, left) + across:
        pl.semaphore_signal(barrier, inc=1, device_id=to, device_id_type=MESH)
    for o in range(1, 8):
        pl.semaphore_signal(barrier, inc=1, device_id=(lax.rem(me + o, n), s), device_id_type=MESH)
    pl.semaphore_wait(barrier, 12)

    mine = pl.ds(pl.multiple_of(x * 256 + y * 128 + c * 64, 64), 64)

    def ag_y(j, i):
        src = (W.at[j, mine], WS.at[j], WS.at[j])[i]
        return send(src, W.at[j, mine], ays.at[j, i], ayr.at[j, i], across[i])

    loads[0].wait()

    def cast(j, _):
        for k in range(2):
            a = pl.ds(pl.multiple_of(k * 2048 + c * 1024 + j * HB, HB), HB)
            b = pl.ds(pl.multiple_of(k * 2048 + (1 - c) * 1024 + j * HB, HB), HB)
            W[j, mine, k * HB : (k + 1) * HB] = mst[:, a].astype(BF)
            WS[j, :, k * HB : (k + 1) * HB] = mst[:, b].astype(BF)
        for i in range(3):
            ag_y(j, i).start()
        return 0

    lax.fori_loop(0, NJ, cast, 0)
    for k, (a, b) in enumerate(((tok, T), (cot, C))):
        for cs, cd in blocks():
            send(a.at[:, cs], b.at[pl.ds(td, td), cd], tks.at[k], tkr.at[k], across[2]).start()
    for cp in loads[1:]:
        cp.start()

    def rows(xx, lo, count):
        return pl.ds(pl.multiple_of(lax.rem(xx, 4) * 256 + lo, 128), count)

    def ag_1(j, i):
        r = rows(x, 0, 256)
        return send(W.at[j, r], W.at[j, r], a1s.at[j, i], a1r.at[j, i], (right, left)[i])

    def ag_1_in(j, i):
        r = rows(x + (3, 1)[i], 0, 256)
        return send(W.at[j, r], W.at[j, r], a1s.at[j, i], a1r.at[j, i], (right, left)[i])

    def ag_2(j, i):
        r = rows(x + (3, 1)[i], (0, 128)[i], 128)
        return send(W.at[j, r], W.at[j, r], a2s.at[j, i], a2r.at[j, i], (right, left)[i])

    def ag_2_in(j, i):
        r = rows(x + 2, (0, 128)[i], 128)
        return send(W.at[j, r], W.at[j, r], a2s.at[j, i], a2r.at[j, i], (right, left)[i])

    def gather_one(j):
        for i in range(3):
            ag_y(j, i).wait_recv()
        for i in range(2):
            ag_1(j, i).start()

    def gather_two(j):
        for i in range(2):
            ag_1_in(j, i).wait_recv()
        for i in range(2):
            ag_2(j, i).start()

    def gather_end(j):
        for i in range(2):
            ag_2_in(j, i).wait_recv()

    def forward(i, _):
        r = pl.ds(pl.multiple_of(i * BT, BT), BT)
        j = _
        pre = jnp.dot(T[r, :], W[j, :, :HB], preferred_element_type=F32)
        back = jnp.dot(C[r, :], W[j, :, HB:], preferred_element_type=F32)
        a, d = gelu_pair(pre, back)
        act[r, :] = a.astype(BF)
        dpre[r, :] = d.astype(BF)
        return _

    def grads(dest):
        q = pl.ds(pl.multiple_of(lax.rem(dest, 4) * 256, 256), 256)
        dims = (((0,), (0,)), ((), ()))
        return (
            lax.dot_general(T[:, q], dpre[...], dims, preferred_element_type=F32),
            lax.dot_general(C[:, q], act[...], dims, preferred_element_type=F32),
        )

    def put(ref, pair, r):
        ref[:, :HB] = pair[0][r].astype(ref.dtype)
        ref[:, HB:] = pair[1][r].astype(ref.dtype)

    upper, lower = slice(0, 128), slice(128, 256)

    def rs(j, i):
        to = right if i in (0, 2, 4) else left
        return send(sb.at[j, i], rb.at[j, i], rss.at[j, i], rsr.at[j, i], to)

    def yc(j, i):
        return send(ys.at[j, i], yr.at[j, i], ycs.at[j, i], ycr.at[j, i], across[i])

    def reduce_one(j):
        for i in range(2):
            rs(j, i).wait_recv()
            sb[j, 4 + i] = (gp[j, i] + rb[j, i].astype(F32)).astype(BF)
            rs(j, 4 + i).start()

    def reduce_two(j):
        for i in (2, 3, 4, 5):
            rs(j, i).wait_recv()
        gx[j, upper] = gx[j, upper] + rb[j, 3].astype(F32) + rb[j, 4].astype(F32)
        gx[j, lower] = gx[j, lower] + rb[j, 2].astype(F32) + rb[j, 5].astype(F32)
        for i, (yy, cc) in enumerate(((1 - y, c), (1 - y, 1 - c), (y, 1 - c))):
            r = pl.ds(pl.multiple_of(yy * 128 + cc * 64, 64), 64)
            ys[j, i] = gx[j, r].astype(BF)
            yc(j, i).start()

    def out_copy(buf, ref, k, j, cols):
        return pltpu.make_async_copy(buf.at[:, cols], ref.at[:, cols], outs.at[k])

    def to_member(buf, slot, j, o, ss, rs_):
        i = lax.rem(me + o, n)
        return send(buf.at[j, slot(i)], (dr if buf is dl else mr).at[j, me], ss, rs_, (i, s))

    def step(j):
        for i in range(3):
            yc(j, i).wait_recv()
        r = pl.ds(pl.multiple_of(y * 128 + c * 64, 64), 64)
        sums = (
            (c, gx[j, r] + yr[j, 0].astype(F32)),
            (1 - c, yr[j, 1].astype(F32) + yr[j, 2].astype(F32)),
        )
        for h, total in sums:
            for k in range(2):
                cols = pl.ds(pl.multiple_of(k * 2048 + h * 1024 + j * HB, HB), HB)
                g = total[:, k * HB : (k + 1) * HB]
                first = 0.9 * b1[:, cols] + 0.1 * g
                second = 0.95 * b2[:, cols] + 0.05 * g * g
                update = first / first_correction / (jnp.sqrt(second / second_correction) + 1e-08)
                p = mst[:, cols]
                inner = p - 0.001 * (update + 0.1 * p)
                delta = ba[:, cols] - inner
                b1[:, cols] = first
                b2[:, cols] = second
                out_copy(b1, o1, 0, j, cols).start()
                out_copy(b2, o2, 1, j, cols).start()
                for t in range(2):
                    dl[j, 4 * h + 2 * k + t] = delta[:, t * 128 : (t + 1) * 128].astype(BF)
        for o in range(1, 8):
            to_member(dl, lambda i: i, j, o, m1s.at[j], m1r.at[j]).start()

    def bytes_of_seven(ref, j, sem):
        seven = ref.at[j, pl.ds(0, 7)]
        return pltpu.make_async_copy(seven, seven, sem)

    def mean(j):
        bytes_of_seven(dr, j, m1r.at[j]).wait()
        total = dl[j, me].astype(F32)
        for o in range(1, 8):
            total = total + dr[j, lax.rem(me + o, n)].astype(F32)
        mr[j, me] = total / n
        for o in range(1, 8):
            to_member(mr, lambda i: me, j, o, m2s.at[j], m2r.at[j]).start()

    def outer(j):
        bytes_of_seven(mr, j, m2r.at[j]).wait()
        for h in range(2):
            for k in range(2):
                for t in range(2):
                    cols = pl.ds(
                        pl.multiple_of(k * 2048 + h * 1024 + j * HB + t * 128, 128), 128
                    )
                    m = mr[j, 4 * h + 2 * k + t]
                    momentum = 0.9 * bo[:, cols] + m
                    bo[:, cols] = momentum
                    ba[:, cols] = ba[:, cols] - 0.7 * (m + 0.9 * momentum)
                cols = pl.ds(pl.multiple_of(k * 2048 + h * 1024 + j * HB, HB), HB)
                out_copy(bo, om, 2, j, cols).start()
                out_copy(ba, oa, 3, j, cols).start()

    gather_one(0)
    gather_one(1)
    gather_two(0)
    gather_one(2)
    half_t = pl.ds(0, td)
    late_t = pl.ds(td, td)
    for k, b in enumerate((T, C)):
        pltpu.make_async_copy(b.at[half_t], b.at[half_t], loc.at[1 + k]).wait()

    def chunk(j, _):
        gather_end(j)
        lax.fori_loop(0, td // BT, forward, j)

        @pl.when(j == 0)
        def _():
            for k, b in enumerate((T, C)):
                pltpu.make_async_copy(b.at[late_t], b.at[late_t], tkr.at[k]).wait()

        @pl.when(j >= 1)
        def _():
            reduce_one(j - 1)

        @pl.when(j < NJ - 1)
        def _():
            gather_two(j + 1)

        @pl.when(j == 0)
        def _():
            gather_one(3)

        lax.fori_loop(td // BT, 2 * td // BT, forward, j)

        @pl.when(j >= 2)
        def _():
            mean(j - 2)

        pair = grads(x + 2)
        put(sb.at[j, 0], pair, upper)
        put(sb.at[j, 1], pair, lower)
        rs(j, 0).start()
        rs(j, 1).start()

        @pl.when(j >= 1)
        def _():
            reduce_two(j - 1)

        pair = grads(x + 1)
        put(gp.at[j, 0], pair, upper)
        put(sb.at[j, 2], pair, lower)
        rs(j, 2).start()
        pair = grads(x + 3)
        put(gp.at[j, 1], pair, lower)
        put(sb.at[j, 3], pair, upper)
        rs(j, 3).start()
        pair = grads(x)
        put(gx.at[j], pair, slice(0, 256))

        @pl.when(j == 1)
        def _():
            for cp in loads[1:]:
                cp.wait()

        @pl.when(j >= 1)
        def _():
            step(j - 1)

        @pl.when(j >= 2)
        def _():
            outer(j - 2)

        return 0

    lax.fori_loop(0, NJ, chunk, 0)
    last = NJ - 1
    reduce_one(last)
    mean(last - 1)
    reduce_two(last)
    outer(last - 1)
    step(last)
    mean(last)
    outer(last)

    def drain(j, _):
        for i in range(3):
            ag_y(j, i).wait_send()
            yc(j, i).wait_send()
        for i in range(2):
            ag_1(j, i).wait_send()
            ag_2(j, i).wait_send()
        for i in range(6):
            rs(j, i).wait_send()
        bytes_of_seven(dl, j, m1s.at[j]).wait()
        bytes_of_seven(mr, j, m2s.at[j]).wait()
        return 0

    lax.fori_loop(0, NJ, drain, 0)
    for k, b in enumerate((T, C)):
        pltpu.make_async_copy(b.at[half_t], b.at[half_t], tks.at[k]).wait()
    for k, (buf, ref) in enumerate(((b1, o1), (b2, o2), (bo, om), (ba, oa))):
        pltpu.make_async_copy(buf, ref, outs.at[k]).wait()


def shards(tokens, cotangent, master, moment_one, moment_two, anchor, outer_momentum):
    td, d = tokens.shape
    r, w = master.shape
    vm = pltpu.VMEM
    dma = pltpu.SemaphoreType.DMA
    wide = jax.ShapeDtypeStruct((r, w), F32)
    any_ = pl.BlockSpec(memory_space=pl.ANY)
    return pl.pallas_call(
        kernel,
        out_shape=(wide,) * 4,
        in_specs=[any_] * 7,
        out_specs=(any_,) * 4,
        scratch_shapes=[
            vm((2 * td, d), BF), vm((2 * td, d), BF), vm((NJ, d, 2 * HB), BF), vm((NJ, r, 2 * HB), BF),
            vm((r, w), F32), vm((r, w), F32), vm((r, w), F32), vm((r, w), F32), vm((r, w), F32),
            vm((2 * td, HB), BF), vm((2 * td, HB), BF),
            vm((NJ, 256, 2 * HB), F32), vm((NJ, 2, 128, 2 * HB), F32),
            vm((NJ, 6, 128, 2 * HB), BF), vm((NJ, 6, 128, 2 * HB), BF),
            vm((NJ, 3, r, 2 * HB), BF), vm((NJ, 3, r, 2 * HB), BF),
            vm((NJ, 8, r, 128), BF), vm((NJ, 8, r, 128), BF), vm((NJ, 8, r, 128), F32),
            dma((7,)), dma((2,)), dma((2,)),
            dma((NJ, 3)), dma((NJ, 3)), dma((NJ, 2)), dma((NJ, 2)), dma((NJ, 2)), dma((NJ, 2)),
            dma((NJ, 6)), dma((NJ, 6)), dma((NJ, 3)), dma((NJ, 3)),
            dma((NJ,)), dma((NJ,)), dma((NJ,)), dma((NJ,)), dma((4,)),
        ],
        compiler_params=pltpu.CompilerParams(
            collective_id=0, has_side_effects=True, vmem_limit_bytes=62 * 1024 * 1024
        ),
        cost_estimate=pl.CostEstimate(
            flops=4 * 2 * td * d * 2048, bytes_accessed=16 << 20, transcendentals=0
        ),
        name="outer_step",
    )(tokens, cotangent, master, moment_one, moment_two, anchor, outer_momentum)


def solution(mesh):
    rows = P(("group", "shard"), None)
    own = P("shard", None)
    return jax.shard_map(
        shards,
        mesh=mesh,
        in_specs=(rows, rows, rows, rows, rows, own, own),
        out_specs=(rows, rows, own, own),
        check_vma=False,
    )
```

```python
import functools
import jax
import jax.numpy as jnp
from jax import lax
from jax.experimental import pallas as pl
from jax.experimental.pallas import tpu as pltpu
from jax.sharding import PartitionSpec as P

first_correction = 0.9999734386011124
second_correction = 0.994079470779664
MESH = pl.DeviceIdType.MESH
BF = jnp.bfloat16
F32 = jnp.float32
NJ = 4
NU = 2 * NJ
HB = 256
VMEM_MIB = 49
BT = 512
ROOT = 0.7978845608028654


def gelu_pair(pre, back):
    square = pre * pre
    t = jnp.tanh(pre * (ROOT + (ROOT * 0.044715) * square))
    half = 0.5 + 0.5 * t
    slope = half + pre * (0.5 * ROOT + (1.5 * ROOT * 0.044715) * square) * (1.0 - t * t)
    return pre * half, back * slope


def kernel(
    tok, cot, mas, mo1, mo2, anc, omo,
    o1, o2, om, oa,
    T, C, W, WS, mst, b1, b2, ba, bo, act, dpre, pool, sb, rb, ys, yr, dl, dr, mr,
    loc, tks, tkr, s1s, s1r, s2s, s2r, rss, rsr, ycs, ycr, m1s, m1r, m2s, m2r, outs,
):
    me = lax.axis_index("group")
    s = lax.axis_index("shard")
    y, x, c = s // 8, (s // 2) % 4, s % 2
    n = lax.axis_size("group")
    td = tok.shape[0]

    def dev(yy, xx, cc):
        return (me, yy * 8 + lax.rem(xx, 4) * 2 + cc)

    right, left = dev(y, x + 1, c), dev(y, x + 3, c)
    across = (dev(1 - y, x, c), dev(1 - y, x, 1 - c), dev(y, x, 1 - c))
    greeted = (right, left) + across + (dev(y, x + 1, 1 - c), dev(y, x + 3, 1 - c))
    first_to = across + (right, left) + greeted[5:]

    def send(src, dst, ss, rs, to):
        return pltpu.make_async_remote_copy(
            src_ref=src, dst_ref=dst, send_sem=ss, recv_sem=rs, device_id=to, device_id_type=MESH
        )

    loads = [pltpu.make_async_copy(mas, mst, loc.at[0])]
    for i, (a, b) in enumerate(((mo1, b1), (mo2, b2), (anc, ba), (omo, bo))):
        loads.append(pltpu.make_async_copy(a, b, loc.at[3 + i]))
    loads[0].start()

    def blocks():
        for k in range(4):
            for yy in range(2):
                at = (yy * 4 + lax.rem(x + k, 4)) * 128
                yield pl.ds(pl.multiple_of(at, 128), 128), slice(k * 256 + yy * 128, k * 256 + yy * 128 + 128)

    for k, (a, b) in enumerate(((tok, T), (cot, C))):
        for cs, cd in blocks():
            pltpu.make_async_copy(a.at[:, cs], b.at[pl.ds(0, td), cd], loc.at[1 + k]).start()

    barrier = pltpu.get_barrier_semaphore()
    for o in range(1, 8):
        pl.semaphore_signal(barrier, inc=1, device_id=(lax.rem(me + o, n), s), device_id_type=MESH)
    for to in greeted:
        pl.semaphore_signal(barrier, inc=1, device_id=to, device_id_type=MESH)

    def rows(k, yy, cc=0, count=64):
        return pl.ds(pl.multiple_of((k % 4) * 256 + yy * 128 + cc * 64, 64), count)

    mine = rows(0, y, c)

    def weight(j, k, sems, src, dst, to):
        ss, rs_ = sems
        return send(src, W.at[j, dst], ss.at[j, k], rs_.at[j, k], to)

    def g1(j, k):
        src = W.at[j, mine] if k in (0, 3, 4) else WS.at[j]
        dst = rows((0, 0, 0, 3, 1, 3, 1)[k], y, c)
        return weight(j, k, (s1s, s1r), src, dst, first_to[k])

    def g2(j, k):
        a, b, yy, cc, count = (
            (0, 3, 1 - y, 0, 128), (0, 1, 1 - y, 0, 128),
            (3, 2, y, 0, 64), (1, 2, y, 1, 64),
            (3, 2, 1 - y, 0, 64), (1, 2, 1 - y, 1, 64),
            (2, 2, y, 0, 128), (3, 3, y, 0, 128), (1, 1, y, 0, 128),
        )[k]
        to = across[0] if k >= 6 else (right, left)[k % 2]
        return weight(j, k, (s2s, s2r), W.at[j, rows(a, yy, cc, count)], rows(b, yy, cc, count), to)

    def arrive(f, j, *ks):
        for k in ks:
            f(j, k).wait_recv()

    def go(f, j, *ks):
        for k in ks:
            f(j, k).start()

    def near_y(j):
        go(g1, j, 0, 1, 2)

    def near_x(j):
        go(g1, j, 3, 4, 5, 6)

    def pass_own(j):
        arrive(g1, j, 3, 5)
        go(g2, j, 2)
        arrive(g1, j, 4, 6)
        go(g2, j, 3)
        if j > 0:
            go(g2, j, 7, 8)

    def pass_other(j):
        arrive(g1, j, 0, 1)
        go(g2, j, 0, 1)

    def pass_far(j):
        if j == 0:
            arrive(g2, j, 0)
            go(g2, j, 4)
            arrive(g2, j, 1)
            go(g2, j, 5)
        else:
            arrive(g2, j, 2, 3)
            go(g2, j, 6)

    def gather_end(j):
        if j == 0:
            arrive(g2, j, 2, 3, 4, 5)
        else:
            arrive(g1, j, 0, 1, 2)
            arrive(g2, j, 7, 8, 6)

    loads[0].wait()

    def cast(j, _):
        for k in range(2):
            a = pl.ds(pl.multiple_of(k * 2048 + c * 1024 + j * HB, HB), HB)
            b = pl.ds(pl.multiple_of(k * 2048 + (1 - c) * 1024 + j * HB, HB), HB)
            W[j, mine, k * HB : (k + 1) * HB] = mst[:, a].astype(BF)
            WS[j, :, k * HB : (k + 1) * HB] = mst[:, b].astype(BF)
        return 0

    lax.fori_loop(0, NJ, cast, 0)
    pl.semaphore_wait(barrier, 14)

    near_y(0)
    near_x(0)
    near_y(1)
    near_x(1)
    near_y(2)
    near_y(3)
    for k, (a, b) in enumerate(((tok, T), (cot, C))):
        for cs, cd in blocks():
            send(a.at[:, cs], b.at[pl.ds(td, td), cd], tks.at[k], tkr.at[k], across[2]).start()
    for cp in loads[1:]:
        cp.start()

    def tile(i):
        return pl.ds(pl.multiple_of(i * BT, BT), BT)

    def finish(r, pre, back):
        a, d = gelu_pair(pre, back)
        act[r, :] = a.astype(BF)
        dpre[r, :] = d.astype(BF)

    def forward(i, j):
        r = slice(i * td, (i + 1) * td)
        pre = jnp.dot(T[r, :], W[j, :, :HB], preferred_element_type=F32)
        back = jnp.dot(C[r, :], W[j, :, HB:], preferred_element_type=F32)
        finish(r, pre, back)

    def product(r, k):
        q = slice(k * 256, k * 256 + 256)
        return (
            jnp.dot(T[r, q], W[0, q, :HB], preferred_element_type=F32),
            jnp.dot(C[r, q], W[0, q, HB:], preferred_element_type=F32),
        )

    def part(i, k):
        return pl.ds(pl.multiple_of(k * 2 * td + i * BT, BT), BT)

    def early(i, _):
        r = tile(i)
        a, b, d = product(r, 0), product(r, 1), product(r, 3)
        for k in range(2):
            pool[part(i, k), :] = a[k] + b[k] + d[k]
        return 0

    def late(i, _):
        r = tile(i)
        a = product(r, 2)
        finish(r, pool[part(i, 0), :] + a[0], pool[part(i, 1), :] + a[1])
        return 0

    half = td // BT
    half_t = pl.ds(0, td)
    late_t = pl.ds(td, td)

    def tokens_own():
        arrive(g1, 0, 2)
        for k, b in enumerate((T, C)):
            pltpu.make_async_copy(b.at[half_t], b.at[half_t], loc.at[1 + k]).wait()

    def tokens_other():
        for k, b in enumerate((T, C)):
            pltpu.make_async_copy(b.at[late_t], b.at[late_t], tkr.at[k]).wait()

    upper, lower = slice(0, 128), slice(128, 256)

    def rs(u, i):
        to = right if i in (0, 2, 4) else left
        return send(sb.at[u, i], rb.at[u, i], rss.at[u, i], rsr.at[u, i], to)

    def yc(u, i):
        return send(ys.at[u, i], yr.at[u, i], ycs.at[u, i], ycr.at[u, i], across[i])

    def gx(u):
        return pool.at[u * 256 : (u + 1) * 256]

    def gp(u, i):
        at = NU * 256 + u * 256 + i * 128
        return pool.at[at : at + 128]

    def grad(u):
        a, b = ((T, dpre), (C, act))[u % 2]
        dims = (((0,), (0,)), ((), ()))
        far = lax.dot_general(a[:, 512:], b[...], dims, preferred_element_type=F32)
        near = lax.dot_general(a[:, :512], b[...], dims, preferred_element_type=F32)
        for i, v in enumerate((far[:128], far[128:256], near[384:], far[256:384])):
            sb[u, i] = v.astype(BF)
        gx(u)[...] = near[:256]
        gp(u, 0)[...] = near[256:384]
        gp(u, 1)[...] = far[384:]
        for i in range(4):
            rs(u, i).start()

    def reduce_one(u):
        for i in range(2):
            rs(u, i).wait_recv()
            sb[u, 4 + i] = (gp(u, i)[...] + rb[u, i].astype(F32)).astype(BF)
            rs(u, 4 + i).start()

    def reduce_two(u):
        for i in (2, 3, 4, 5):
            rs(u, i).wait_recv()
        for r, a, b in ((upper, 3, 4), (lower, 2, 5)):
            gx(u)[r] = gx(u)[r] + rb[u, a].astype(F32) + rb[u, b].astype(F32)
        for i, (yy, cc) in enumerate(((1 - y, c), (1 - y, 1 - c), (y, 1 - c))):
            r = pl.ds(pl.multiple_of(yy * 128 + cc * 64, 64), 64)
            ys[u, i] = gx(u)[r].astype(BF)
            yc(u, i).start()

    def out_copy(buf, ref, k, cols):
        return pltpu.make_async_copy(buf.at[:, cols], ref.at[:, cols], outs.at[k])

    def columns(u, h):
        j, k = u // 2, u % 2
        return pl.ds(pl.multiple_of(k * 2048 + h * 1024 + j * HB, HB), HB)

    def eight(i):
        return pl.ds(pl.multiple_of(i * 8, 8), 8)

    def send_delta(u, o):
        i = lax.rem(me + o, n)
        return send(dl.at[u, eight(i)], dr.at[u, eight(me)], m1s.at[u], m1r.at[u], (i, s))

    def send_mean(u, o):
        i = lax.rem(me + o, n)
        return send(mr.at[u, eight(me)], mr.at[u, eight(me)], m2s.at[u], m2r.at[u], (i, s))

    def step(u):
        for i in range(3):
            yc(u, i).wait_recv()
        r = pl.ds(pl.multiple_of(y * 128 + c * 64, 64), 64)
        sums = (
            (c, gx(u)[r] + yr[u, 0].astype(F32)),
            (1 - c, yr[u, 1].astype(F32) + yr[u, 2].astype(F32)),
        )
        for h, g in sums:
            cols = columns(u, h)
            first = 0.9 * b1[:, cols] + 0.1 * g
            second = 0.95 * b2[:, cols] + 0.05 * g * g
            root = jnp.sqrt(second * (1.0 / second_correction)) + 1e-08
            update = first * (1.0 / first_correction) / root
            p = mst[:, cols]
            inner = p - 0.001 * (update + 0.1 * p)
            b1[:, cols] = first
            b2[:, cols] = second
            out_copy(b1, o1, 0, cols).start()
            out_copy(b2, o2, 1, cols).start()
            dl[u, :, pl.ds(pl.multiple_of(h * HB, HB), HB)] = ba[:, cols] - inner
        for o in range(1, 8):
            send_delta(u, o).start()

    def seven(ref, u, sem):
        part_ = ref.at[u, pl.ds(0, 56)]
        return pltpu.make_async_copy(part_, part_, sem)

    def mean(u):
        seven(dr, u, m1r.at[u]).wait()
        total = dl[u, eight(me)]
        for o in range(1, 8):
            total = total + dr[u, eight(lax.rem(me + o, n))]
        mr[u, eight(me)] = total / n
        for o in range(1, 8):
            send_mean(u, o).start()

    def outer(u):
        seven(mr, u, m2r.at[u]).wait()
        for h in range(2):
            cols = columns(u, h)
            m = mr[u, :, h * HB : (h + 1) * HB]
            momentum = 0.9 * bo[:, cols] + m
            bo[:, cols] = momentum
            ba[:, cols] = ba[:, cols] - 0.7 * (m + 0.9 * momentum)
            out_copy(bo, om, 2, cols).start()
            out_copy(ba, oa, 3, cols).start()

    pass_other(0)
    pass_own(0)
    pass_own(1)
    pass_far(0)
    near_x(2)
    tokens_own()
    lax.fori_loop(0, half, early, 0)
    tokens_other()
    lax.fori_loop(half, 2 * half, early, 0)
    pass_far(1)
    near_x(3)
    gather_end(0)
    lax.fori_loop(0, 2 * half, late, 0)
    pass_own(2)

    def both(f, j):
        if 0 <= j < NJ:
            f(2 * j + 1)
            f(2 * j)

    for j in range(NJ):
        if j > 0:
            gather_end(j)
            forward(0, j)
            if j == 2:
                for cp in loads[1:]:
                    cp.wait()
            both(reduce_two, j - 2)
            forward(1, j)
            if j == 1:
                pass_far(3)
            both(reduce_one, j - 1)
            both(mean, j - 3)
        grad(2 * j + 1)
        if j == 0:
            pass_own(3)
        grad(2 * j)
        if j == 0:
            pass_far(2)
        both(step, j - 2)
        both(outer, j - 3)

    p, q = NU - 2, NU - 1
    both(reduce_two, NJ - 2)
    reduce_one(q)
    reduce_one(p)
    both(mean, NJ - 3)
    both(step, NJ - 2)
    reduce_two(q)
    reduce_two(p)
    both(outer, NJ - 3)
    both(mean, NJ - 2)
    step(q)
    step(p)
    both(outer, NJ - 2)
    mean(q)
    mean(p)
    outer(q)
    outer(p)

    def drain(j, _):
        for k in range(7):
            g1(j, k).wait_send()
        for k in (2, 3):
            g2(j, k).wait_send()
        return 0

    def drain_sums(u, _):
        for i in range(3):
            yc(u, i).wait_send()
        for i in range(6):
            rs(u, i).wait_send()
        seven(dl, u, m1s.at[u]).wait()
        seven(mr, u, m2s.at[u]).wait()
        return 0

    lax.fori_loop(0, NJ, drain, 0)
    for j in range(NJ):
        for k in (6, 7, 8) if j else (0, 1, 4, 5):
            g2(j, k).wait_send()
    lax.fori_loop(0, NU, drain_sums, 0)
    for k, b in enumerate((T, C)):
        pltpu.make_async_copy(b.at[half_t], b.at[half_t], tks.at[k]).wait()
    for k, (buf, ref) in enumerate(((b1, o1), (b2, o2), (bo, om), (ba, oa))):
        pltpu.make_async_copy(buf, ref, outs.at[k]).wait()


def shards(tokens, cotangent, master, moment_one, moment_two, anchor, outer_momentum):
    td, d = tokens.shape
    r, w = master.shape
    vm = pltpu.VMEM
    dma = pltpu.SemaphoreType.DMA
    wide = jax.ShapeDtypeStruct((r, w), F32)
    return pl.pallas_call(
        kernel,
        out_shape=(wide,) * 4,
        in_specs=[pl.BlockSpec(memory_space=pltpu.HBM)] * 7,
        out_specs=(pl.BlockSpec(memory_space=pl.ANY),) * 4,
        scratch_shapes=[
            vm((2 * td, d), BF), vm((2 * td, d), BF), vm((NJ, d, 2 * HB), BF), vm((NJ, r, 2 * HB), BF),
            vm((r, w), F32), vm((r, w), F32), vm((r, w), F32), vm((r, w), F32), vm((r, w), F32),
            vm((2 * td, HB), BF), vm((2 * td, HB), BF), vm((4 * td, HB), F32),
            vm((NU, 6, 128, HB), BF), vm((NU, 6, 128, HB), BF),
            vm((NU, 3, r, HB), BF), vm((NU, 3, r, HB), BF),
            vm((NU, r, 2 * HB), F32), vm((NU, r, 2 * HB), F32), vm((NU, r, 2 * HB), F32),
            dma((7,)), dma((2,)), dma((2,)),
            dma((NJ, 7)), dma((NJ, 7)), dma((NJ, 9)), dma((NJ, 9)),
            dma((NU, 6)), dma((NU, 6)), dma((NU, 3)), dma((NU, 3)),
            dma((NU,)), dma((NU,)), dma((NU,)), dma((NU,)), dma((4,)),
        ],
        compiler_params=pltpu.CompilerParams(
            collective_id=0, has_side_effects=True, vmem_limit_bytes=VMEM_MIB * 1024 * 1024
        ),
        cost_estimate=pl.CostEstimate(
            flops=4 * 2 * td * d * 2048, bytes_accessed=16 << 20, transcendentals=0
        ),
        name="outer_step",
    )(tokens, cotangent, master, moment_one, moment_two, anchor, outer_momentum)


def solution(mesh):
    rows = P(("group", "shard"), None)
    own = P("shard", None)
    return jax.shard_map(
        shards,
        mesh=mesh,
        in_specs=(rows, rows, rows, rows, rows, own, own),
        out_specs=(rows, rows, own, own),
        check_vma=False,
    )
```

```python
import functools
import jax
import jax.numpy as jnp
from jax import lax
from jax.experimental import pallas as pl
from jax.experimental.pallas import tpu as pltpu
from jax.sharding import PartitionSpec as P

first_correction = 0.9999734386011124
second_correction = 0.994079470779664
MESH = pl.DeviceIdType.MESH
BF = jnp.bfloat16
F32 = jnp.float32
NJ = 4
NU = 2 * NJ
HB = 256
VMEM_MIB = 49
BT = 512
ROOT = 0.7978845608028654


def gelu_pair(pre):
    square = pre * pre
    t = jnp.tanh(pre * (ROOT + (ROOT * 0.044715) * square))
    half = 0.5 + 0.5 * t
    slope = half + pre * (0.5 * ROOT + (1.5 * ROOT * 0.044715) * square) * (1.0 - t * t)
    return pre * half, slope


def kernel(
    tok, cot, mas, mo1, mo2, anc, omo,
    o1, o2, om, oa,
    T, C, W, WS, mst, b1, b2, ba, bo, act, dpre, slope, pool, sb, rb, ys, yr, dl, dr, mr,
    loc, tks, tkr, s1s, s1r, s2s, s2r, rss, rsr, ycs, ycr, m1s, m1r, m2s, m2r, outs,
):
    me = lax.axis_index("group")
    s = lax.axis_index("shard")
    y, x, c = s // 8, (s // 2) % 4, s % 2
    n = lax.axis_size("group")
    td = tok.shape[0]

    def dev(yy, xx, cc):
        return (me, yy * 8 + lax.rem(xx, 4) * 2 + cc)

    right, left = dev(y, x + 1, c), dev(y, x + 3, c)
    across = (dev(1 - y, x, c), dev(1 - y, x, 1 - c), dev(y, x, 1 - c))
    greeted = (right, left) + across + (dev(y, x + 1, 1 - c), dev(y, x + 3, 1 - c))
    first_to = across + (right, left) + greeted[5:]

    def send(src, dst, ss, rs, to):
        return pltpu.make_async_remote_copy(
            src_ref=src, dst_ref=dst, send_sem=ss, recv_sem=rs, device_id=to, device_id_type=MESH
        )

    loads = [pltpu.make_async_copy(mas, mst, loc.at[0])]
    for i, (a, b) in enumerate(((mo1, b1), (mo2, b2), (anc, ba), (omo, bo))):
        loads.append(pltpu.make_async_copy(a, b, loc.at[3 + i]))
    loads[0].start()

    def blocks():
        for k in range(4):
            for yy in range(2):
                at = (yy * 4 + lax.rem(x + k, 4)) * 128
                yield pl.ds(pl.multiple_of(at, 128), 128), slice(k * 256 + yy * 128, k * 256 + yy * 128 + 128)

    for k, (a, b) in enumerate(((tok, T), (cot, C))):
        for cs, cd in blocks():
            pltpu.make_async_copy(a.at[:, cs], b.at[pl.ds(0, td), cd], loc.at[1 + k]).start()

    barrier = pltpu.get_barrier_semaphore()
    for o in range(1, 8):
        pl.semaphore_signal(barrier, inc=1, device_id=(lax.rem(me + o, n), s), device_id_type=MESH)
    for to in greeted:
        pl.semaphore_signal(barrier, inc=1, device_id=to, device_id_type=MESH)

    def rows(k, yy, cc=0, count=64):
        return pl.ds(pl.multiple_of((k % 4) * 256 + yy * 128 + cc * 64, 64), count)

    mine = rows(0, y, c)

    def weight(j, k, sems, src, dst, to):
        ss, rs_ = sems
        return send(src, W.at[j, dst], ss.at[0], rs_.at[j, k], to)

    def g1(j, k):
        src = W.at[j, mine] if k in (0, 3, 4) else WS.at[j]
        dst = rows((0, 0, 0, 3, 1, 3, 1)[k], y, c)
        return weight(j, (0, 0, 0, 1, 2, 1, 2)[k], (s1s, s1r), src, dst, first_to[k])

    def g2(j, k):
        a, b, yy, cc, count = (
            (0, 3, 1 - y, 0, 128), (0, 1, 1 - y, 0, 128),
            (3, 2, y, 0, 64), (1, 2, y, 1, 64),
            (3, 2, 1 - y, 0, 64), (1, 2, 1 - y, 1, 64),
            (2, 2, y, 0, 128), (3, 3, y, 0, 128), (1, 1, y, 0, 128),
        )[k]
        to = across[0] if k >= 6 else (right, left)[k % 2]
        i = (0, 1, 2, 2, 2, 2)[k] if j == 0 else (0, 0, 0, 0, 0, 0, 1, 1, 1)[k]
        return weight(j, i, (s2s, s2r), W.at[j, rows(a, yy, cc, count)], rows(b, yy, cc, count), to)

    def arrive(sem, count):
        some = W.at[0, pl.ds(0, count)]
        pltpu.make_async_copy(some, some, sem).wait()

    def go(f, j, *ks):
        for k in ks:
            f(j, k).start()

    def near_y(j):
        go(g1, j, 0, 1, 2)

    def near_x(j):
        go(g1, j, 3, 4, 5, 6)

    def pass_own(j):
        arrive(s1r.at[j, 1], 128)
        go(g2, j, 2)
        arrive(s1r.at[j, 2], 128)
        go(g2, j, 3)

    def pass_along_y(j):
        go(g2, j, 7, 8)

    def pass_other(j):
        arrive(s1r.at[j, 0], 192)
        go(g2, j, 0, 1)

    def pass_far(j):
        if j == 0:
            arrive(s2r.at[j, 0], 128)
            go(g2, j, 4)
            arrive(s2r.at[j, 1], 128)
            go(g2, j, 5)
        else:
            arrive(s2r.at[j, 0], 128)
            go(g2, j, 6)

    def gather_end(j):
        if j == 0:
            arrive(s2r.at[j, 2], 256)
        else:
            arrive(s1r.at[j, 0], 192)
            arrive(s2r.at[j, 1], 384)

    loads[0].wait()

    def cast(j, _):
        for k in range(2):
            a = pl.ds(pl.multiple_of(k * 2048 + c * 1024 + j * HB, HB), HB)
            b = pl.ds(pl.multiple_of(k * 2048 + (1 - c) * 1024 + j * HB, HB), HB)
            W[j, mine, k * HB : (k + 1) * HB] = mst[:, a].astype(BF)
            WS[j, :, k * HB : (k + 1) * HB] = mst[:, b].astype(BF)
        return 0

    lax.fori_loop(0, NJ, cast, 0)
    pl.semaphore_wait(barrier, 14)

    near_y(0)
    near_x(0)
    near_y(1)
    near_x(1)
    for k, (a, b) in enumerate(((tok, T), (cot, C))):
        for cs, cd in blocks():
            send(a.at[:, cs], b.at[pl.ds(td, td), cd], tks.at[k], tkr.at[k], across[2]).start()
    for cp in loads[1:]:
        cp.start()

    def tile(i):
        return pl.ds(pl.multiple_of(i * BT, BT), BT)

    def finish(r, pre, back):
        a, d = gelu_pair(pre)
        act[r, :] = a.astype(BF)
        dpre[r, :] = (back * d).astype(BF)

    def forward(i, j):
        r = slice(i * td, (i + 1) * td)
        pre = jnp.dot(T[r, :], W[j, :, :HB], preferred_element_type=F32)
        back = jnp.dot(C[r, :], W[j, :, HB:], preferred_element_type=F32)
        finish(r, pre, back)

    halves = (slice(0, td), slice(td, 2 * td))

    def forward_in(j):
        pre = [jnp.dot(T[r, :], W[j, :, :HB], preferred_element_type=F32) for r in halves]
        for r, v in zip(halves, pre):
            a, d = gelu_pair(v)
            act[r, :] = a.astype(BF)
            slope[r, :] = d

    def forward_out(j):
        back = [jnp.dot(C[r, :], W[j, :, HB:], preferred_element_type=F32) for r in halves]
        for r, v in zip(halves, back):
            dpre[r, :] = (v * slope[r, :]).astype(BF)

    def product(r, k):
        q = slice(k * 256, k * 256 + 256)
        return (
            jnp.dot(T[r, q], W[0, q, :HB], preferred_element_type=F32),
            jnp.dot(C[r, q], W[0, q, HB:], preferred_element_type=F32),
        )

    def part(i, k):
        return pl.ds(pl.multiple_of(k * 2 * td + i * BT, BT), BT)

    def early(i, _):
        r = tile(i)
        a, b, d = product(r, 0), product(r, 1), product(r, 3)
        for k in range(2):
            pool[part(i, k), :] = a[k] + b[k] + d[k]
        return 0

    def late(i, _):
        r = tile(i)
        a = product(r, 2)
        finish(r, pool[part(i, 0), :] + a[0], pool[part(i, 1), :] + a[1])
        return 0

    half = td // BT
    half_t = pl.ds(0, td)
    late_t = pl.ds(td, td)

    def tokens_own():
        for k, b in enumerate((T, C)):
            pltpu.make_async_copy(b.at[half_t], b.at[half_t], loc.at[1 + k]).wait()

    def tokens_other():
        for k, b in enumerate((T, C)):
            pltpu.make_async_copy(b.at[late_t], b.at[late_t], tkr.at[k]).wait()

    upper, lower = slice(0, 128), slice(128, 256)

    def rs(u, i):
        to = right if i in (0, 2, 4) else left
        return send(sb.at[u, i], rb.at[u, i], rss.at[0], rsr.at[u, min(i, 2)], to)

    def yc(u, i):
        return send(ys.at[u, i], yr.at[u, i], ycs.at[0], ycr.at[u], across[i])

    def gx(u):
        return pool.at[u * 256 : (u + 1) * 256]

    def gp(u, i):
        at = NU * 256 + u * 256 + i * 128
        return pool.at[at : at + 128]

    def grad(u, ready=lambda: None, sent=lambda: None):
        a, b = ((T, dpre), (C, act))[u % 2]
        dims = (((0,), (0,)), ((), ()))
        far = lax.dot_general(a[:, 512:], b[...], dims, preferred_element_type=F32)
        near = lax.dot_general(a[:, :512], b[...], dims, preferred_element_type=F32)
        for i, v in enumerate((far[:128], far[128:256], near[384:], far[256:384])):
            sb[u, i] = v.astype(BF)
        gx(u)[...] = near[:256]
        gp(u, 0)[...] = near[256:384]
        gp(u, 1)[...] = far[384:]
        ready()
        for i in range(2):
            rs(u, i).start()
        sent()
        for i in range(2, 4):
            rs(u, i).start()

    def whole(ref, sem):
        pltpu.make_async_copy(ref, ref, sem).wait()

    def reduce_one(u):
        for i in range(2):
            rs(u, i).wait_recv()
            sb[u, 4 + i] = (gp(u, i)[...] + rb[u, i].astype(F32)).astype(BF)
            rs(u, 4 + i).start()

    def reduce_two(u):
        whole(rb.at[u, pl.ds(2, 4)], rsr.at[u, 2])
        for r, a, b in ((upper, 3, 4), (lower, 2, 5)):
            gx(u)[r] = gx(u)[r] + rb[u, a].astype(F32) + rb[u, b].astype(F32)
        for i, (yy, cc) in enumerate(((1 - y, c), (1 - y, 1 - c), (y, 1 - c))):
            r = pl.ds(pl.multiple_of(yy * 128 + cc * 64, 64), 64)
            ys[u, i] = gx(u)[r].astype(BF)
            yc(u, i).start()

    def out_copy(buf, ref, k, cols):
        return pltpu.make_async_copy(buf.at[:, cols], ref.at[:, cols], outs.at[k])

    def columns(u, h):
        j, k = u // 2, u % 2
        return pl.ds(pl.multiple_of(k * 2048 + h * 1024 + j * HB, HB), HB)

    def piece(i):
        return slice(i % 2 * 32, i % 2 * 32 + 32), slice(i // 2 * 128, i // 2 * 128 + 128)

    def send_delta(u, o):
        i = lax.rem(me + o, n)
        return send(dl.at[u, i], dr.at[u, me], m1s.at[0], m1r.at[u], (i, s))

    def send_mean(u, o):
        i = lax.rem(me + o, n)
        return send(mr.at[u, me], mr.at[u, me], m2s.at[0], m2r.at[u], (i, s))

    def step(u):
        whole(yr.at[u], ycr.at[u])
        r = pl.ds(pl.multiple_of(y * 128 + c * 64, 64), 64)
        sums = (
            (c, gx(u)[r] + yr[u, 0].astype(F32)),
            (1 - c, yr[u, 1].astype(F32) + yr[u, 2].astype(F32)),
        )
        for h, g in sums:
            cols = columns(u, h)
            first = 0.9 * b1[:, cols] + 0.1 * g
            second = 0.95 * b2[:, cols] + 0.05 * g * g
            root = jnp.sqrt(second * (1.0 / second_correction)) + 1e-08
            update = first * (1.0 / first_correction) / root
            p = mst[:, cols]
            inner = p - 0.001 * (update + 0.1 * p)
            b1[:, cols] = first
            b2[:, cols] = second
            out_copy(b1, o1, 0, cols).start()
            out_copy(b2, o2, 1, cols).start()
            delta = (ba[:, cols] - inner).astype(BF)
            for i in range(4):
                dl[u, 4 * h + i] = delta[piece(i)]
        for o in range(1, 8):
            send_delta(u, o).start()

    def mean(u):
        whole(dr.at[u, pl.ds(0, 7)], m1r.at[u])
        total = dl[u, me].astype(F32)
        for o in range(1, 8):
            total = total + dr[u, lax.rem(me + o, n)].astype(F32)
        mr[u, me] = total / n
        for o in range(1, 8):
            send_mean(u, o).start()

    def outer(u):
        whole(mr.at[u, pl.ds(0, 7)], m2r.at[u])
        for h in range(2):
            cols = columns(u, h)
            start = u % 2 * 2048 + h * 1024 + u // 2 * HB
            for i in range(4):
                r, q_ = piece(i)
                q_ = slice(start + q_.start, start + q_.stop)
                m = mr[u, 4 * h + i]
                momentum = 0.9 * bo[r, q_] + m
                bo[r, q_] = momentum
                ba[r, q_] = ba[r, q_] - 0.7 * (m + 0.9 * momentum)
            out_copy(bo, om, 2, cols).start()
            out_copy(ba, oa, 3, cols).start()

    pass_other(0)
    pass_own(0)
    pass_own(1)
    pass_along_y(1)
    near_y(2)
    pass_far(0)
    near_x(2)
    tokens_own()
    lax.fori_loop(0, half, early, 0)
    tokens_other()
    lax.fori_loop(half, 2 * half, early, 0)
    pass_far(1)
    near_x(3)
    gather_end(0)
    lax.fori_loop(0, 2 * half, late, 0)

    def second():
        pass_own(2)
        pass_along_y(2)

    grad(1, ready=second)

    def third():
        pass_far(2)
        near_y(3)
        pass_own(3)
        pass_along_y(3)

    grad(0, ready=third)

    def at(f, j, k):
        if j >= 0:
            f(2 * j + k)

    p, q = NU - 2, NU - 1
    for j in range(1, NJ):
        gather_end(j)
        forward_in(j)
        at(reduce_one, j - 1, 1)
        at(reduce_two, j - 2, 0)
        at(mean, j - 3, 1)
        at(step, j - 3, 0)
        grad(2 * j + 1)
        if j == 1:
            pass_far(3)
        forward_out(j)
        if j == 2:
            for cp in loads[1:]:
                cp.wait()
        at(reduce_one, j - 1, 0)
        if j == NJ - 1:
            at(step, j - 2, 1)
        if j < NJ - 1:
            grad(2 * j)
        else:
            grad(2 * j, sent=lambda: reduce_one(q))
        at(reduce_two, j - 1, 1)
        if j < NJ - 1:
            at(step, j - 2, 1)
        else:
            at(mean, j - 3, 0)
            at(step, j - 2, 0)
        at(outer, j - 3, 1)

    reduce_one(p)
    at(outer, NJ - 4, 0)
    reduce_two(p - 2)
    mean(q - 4)
    reduce_two(q)
    step(q - 2)
    mean(p - 4)
    reduce_two(p)
    step(p - 2)
    step(q)
    mean(q - 2)
    step(p)
    outer(q - 4)
    outer(p - 4)
    mean(p - 2)
    mean(q)
    mean(p)
    outer(q - 2)
    outer(p - 2)
    outer(q)
    outer(p)

    whole(W.at[:, pl.ds(0, 7 * 64)], s1s.at[0])
    whole(W.at[:, pl.ds(0, 512)], s2s.at[0])
    whole(sb, rss.at[0])
    whole(ys, ycs.at[0])
    whole(dl.at[pl.ds(0, NU - 1)], m1s.at[0])
    whole(mr.at[pl.ds(0, NU - 1)], m2s.at[0])
    for k, b in enumerate((T, C)):
        pltpu.make_async_copy(b.at[half_t], b.at[half_t], tks.at[k]).wait()
    for k, (buf, ref) in enumerate(((b1, o1), (b2, o2), (bo, om), (ba, oa))):
        pltpu.make_async_copy(buf, ref, outs.at[k]).wait()


def write(a, b, c, d, o1, o2, o3, o4, sems):
    pairs = ((a, o1), (b, o2), (c, o3), (d, o4))
    for wait in (False, True):
        for i, (src, dst) in enumerate(pairs):
            copy = pltpu.make_async_copy(src, dst, sems.at[i])
            copy.wait() if wait else copy.start()


def shards(tokens, cotangent, master, moment_one, moment_two, anchor, outer_momentum):
    td, d = tokens.shape
    r, w = master.shape
    vm = pltpu.VMEM
    dma = pltpu.SemaphoreType.DMA
    wide = jax.ShapeDtypeStruct((r, w), F32)
    results = pl.pallas_call(
        kernel,
        out_shape=(wide,) * 4,
        in_specs=[pl.BlockSpec(memory_space=pltpu.HBM)] * 7,
        out_specs=(pl.BlockSpec(memory_space=pl.ANY),) * 4,
        scratch_shapes=[
            vm((2 * td, d), BF), vm((2 * td, d), BF), vm((NJ, d, 2 * HB), BF), vm((NJ, r, 2 * HB), BF),
            vm((r, w), F32), vm((r, w), F32), vm((r, w), F32), vm((r, w), F32), vm((r, w), F32),
            vm((2 * td, HB), BF), vm((2 * td, HB), BF), vm((2 * td, HB), F32), vm((4 * td, HB), F32),
            vm((NU, 6, 128, HB), BF), vm((NU, 6, 128, HB), BF),
            vm((NU, 3, r, HB), BF), vm((NU, 3, r, HB), BF),
            vm((NU, 8, 32, 128), BF), vm((NU, 8, 32, 128), BF), vm((NU, 8, 32, 128), F32),
            dma((7,)), dma((2,)), dma((2,)),
            dma((1,)), dma((NJ, 3)), dma((1,)), dma((NJ, 3)),
            dma((1,)), dma((NU, 3)), dma((1,)), dma((NU,)),
            dma((1,)), dma((NU,)), dma((1,)), dma((NU,)), dma((4,)),
        ],
        compiler_params=pltpu.CompilerParams(
            collective_id=0, has_side_effects=True, vmem_limit_bytes=VMEM_MIB * 1024 * 1024
        ),
        cost_estimate=pl.CostEstimate(
            flops=4 * 2 * td * d * 2048, bytes_accessed=16 << 20, transcendentals=0
        ),
        name="outer_step",
    )(tokens, cotangent, master, moment_one, moment_two, anchor, outer_momentum)
    return pl.pallas_call(
        write,
        out_shape=(wide,) * 4,
        in_specs=[pl.BlockSpec(memory_space=pl.ANY)] * 4,
        out_specs=(pl.BlockSpec(memory_space=pltpu.HBM),) * 4,
        scratch_shapes=[dma((4,))],
        compiler_params=pltpu.CompilerParams(vmem_limit_bytes=1024 * 1024),
        name="write_results",
    )(*results)


def solution(mesh):
    rows = P(("group", "shard"), None)
    own = P("shard", None)
    return jax.shard_map(
        shards,
        mesh=mesh,
        in_specs=(rows, rows, rows, rows, rows, own, own),
        out_specs=(rows, rows, own, own),
        check_vma=False,
    )
```

```python
import functools
import jax
import jax.numpy as jnp
from jax import lax
from jax.experimental import pallas as pl
from jax.experimental.pallas import tpu as pltpu
from jax.sharding import PartitionSpec as P

first_correction = 0.9999734386011124
second_correction = 0.994079470779664
MESH = pl.DeviceIdType.MESH
BF = jnp.bfloat16
F32 = jnp.float32
NJ = 4
NU = 2 * NJ
HB = 256
VMEM_MIB = 49
BT = 512
ROOT = 0.7978845608028654


def gelu_pair(pre):
    square = pre * pre
    t = jnp.tanh(pre * (ROOT + (ROOT * 0.044715) * square))
    half = 0.5 + 0.5 * t
    slope = half + pre * (0.5 * ROOT + (1.5 * ROOT * 0.044715) * square) * (1.0 - t * t)
    return pre * half, slope


def kernel(
    tok, cot, mas, mo1, mo2, anc, omo,
    o1, o2, om, oa,
    T, C, W, WS, mst, b1, b2, ba, bo, act, dpre, slope, pool, sb, rb, ys, yr, dl, dr, mr,
    loc, tks, tkr, s1s, s1r, s2s, s2r, rss, rsr, ycs, ycr, m1s, m1r, m2s, m2r, outs,
):
    me = lax.axis_index("group")
    s = lax.axis_index("shard")
    y, x, c = s // 8, (s // 2) % 4, s % 2
    n = lax.axis_size("group")
    td = tok.shape[0]

    def dev(yy, xx, cc):
        return (me, yy * 8 + lax.rem(xx, 4) * 2 + cc)

    right, left = dev(y, x + 1, c), dev(y, x + 3, c)
    across = (dev(1 - y, x, c), dev(1 - y, x, 1 - c), dev(y, x, 1 - c))
    greeted = (right, left) + across + (dev(y, x + 1, 1 - c), dev(y, x + 3, 1 - c))
    first_to = across + (right, left) + greeted[5:]

    def send(src, dst, ss, rs, to):
        return pltpu.make_async_remote_copy(
            src_ref=src, dst_ref=dst, send_sem=ss, recv_sem=rs, device_id=to, device_id_type=MESH
        )

    loads = [pltpu.make_async_copy(mas, mst, loc.at[0])]
    for i, (a, b) in enumerate(((mo1, b1), (mo2, b2), (anc, ba), (omo, bo))):
        loads.append(pltpu.make_async_copy(a, b, loc.at[3 + i]))
    loads[0].start()

    def blocks():
        for k in range(4):
            for yy in range(2):
                at = (yy * 4 + lax.rem(x + k, 4)) * 128
                yield pl.ds(pl.multiple_of(at, 128), 128), slice(k * 256 + yy * 128, k * 256 + yy * 128 + 128)

    for k, (a, b) in enumerate(((tok, T), (cot, C))):
        for cs, cd in blocks():
            pltpu.make_async_copy(a.at[:, cs], b.at[pl.ds(0, td), cd], loc.at[1 + k]).start()

    barrier = pltpu.get_barrier_semaphore()
    for o in range(1, 8):
        pl.semaphore_signal(barrier, inc=1, device_id=(lax.rem(me + o, n), s), device_id_type=MESH)
    for to in greeted:
        pl.semaphore_signal(barrier, inc=1, device_id=to, device_id_type=MESH)

    def rows(k, yy, cc=0, count=64):
        return pl.ds(pl.multiple_of((k % 4) * 256 + yy * 128 + cc * 64, 64), count)

    mine = rows(0, y, c)

    def weight(j, k, sems, src, dst, to):
        ss, rs_ = sems
        return send(src, W.at[j, dst], ss.at[0], rs_.at[j, k], to)

    def g1(j, k):
        src = W.at[j, mine] if k in (0, 3, 4) else WS.at[j]
        dst = rows((0, 0, 0, 3, 1, 3, 1)[k], y, c)
        return weight(j, (0, 0, 0, 1, 2, 1, 2)[k], (s1s, s1r), src, dst, first_to[k])

    def g2(j, k):
        a, b, yy, cc, count = (
            (0, 3, 1 - y, 0, 128), (0, 1, 1 - y, 0, 128),
            (3, 2, y, 0, 64), (1, 2, y, 1, 64),
            (3, 2, 1 - y, 0, 64), (1, 2, 1 - y, 1, 64),
            (2, 2, y, 0, 128), (3, 3, y, 0, 128), (1, 1, y, 0, 128),
        )[k]
        to = across[0] if k >= 6 else (right, left)[k % 2]
        i = (0, 1, 2, 2, 2, 2)[k] if j == 0 else (0, 0, 0, 0, 0, 0, 1, 1, 1)[k]
        return weight(j, i, (s2s, s2r), W.at[j, rows(a, yy, cc, count)], rows(b, yy, cc, count), to)

    def arrive(sem, count):
        some = W.at[0, pl.ds(0, count)]
        pltpu.make_async_copy(some, some, sem).wait()

    def go(f, j, *ks):
        for k in ks:
            f(j, k).start()

    def near_y(j):
        go(g1, j, 0, 1, 2)

    def near_x(j):
        go(g1, j, 3, 4, 5, 6)

    def pass_own(j):
        arrive(s1r.at[j, 1], 128)
        go(g2, j, 2)
        arrive(s1r.at[j, 2], 128)
        go(g2, j, 3)

    def pass_along_y(j):
        go(g2, j, 7, 8)

    def pass_other(j):
        arrive(s1r.at[j, 0], 192)
        go(g2, j, 0, 1)

    def pass_far(j):
        if j == 0:
            arrive(s2r.at[j, 0], 128)
            go(g2, j, 4)
            arrive(s2r.at[j, 1], 128)
            go(g2, j, 5)
        else:
            arrive(s2r.at[j, 0], 128)
            go(g2, j, 6)

    def gather_end(j):
        if j == 0:
            arrive(s2r.at[j, 2], 256)
        else:
            arrive(s1r.at[j, 0], 192)
            arrive(s2r.at[j, 1], 384)

    loads[0].wait()

    def cast(j, _):
        for k in range(2):
            a = pl.ds(pl.multiple_of(k * 2048 + c * 1024 + j * HB, HB), HB)
            b = pl.ds(pl.multiple_of(k * 2048 + (1 - c) * 1024 + j * HB, HB), HB)
            W[j, mine, k * HB : (k + 1) * HB] = mst[:, a].astype(BF)
            WS[j, :, k * HB : (k + 1) * HB] = mst[:, b].astype(BF)
        return 0

    lax.fori_loop(0, NJ, cast, 0)
    pl.semaphore_wait(barrier, 14)

    near_y(0)
    near_x(0)
    near_y(1)
    near_x(1)
    near_y(2)
    for k, (a, b) in enumerate(((tok, T), (cot, C))):
        for cs, cd in blocks():
            send(a.at[:, cs], b.at[pl.ds(td, td), cd], tks.at[k], tkr.at[k], across[2]).start()
    for cp in loads[1:]:
        cp.start()

    def tile(i):
        return pl.ds(pl.multiple_of(i * BT, BT), BT)

    def finish(r, pre, back):
        a, d = gelu_pair(pre)
        act[r, :] = a.astype(BF)
        dpre[r, :] = (back * d).astype(BF)

    halves = (slice(0, td), slice(td, 2 * td))

    def forward(i, j):
        r = halves[i]
        pre = jnp.dot(T[r, :], W[j, :, :HB], preferred_element_type=F32)
        back = jnp.dot(C[r, :], W[j, :, HB:], preferred_element_type=F32)
        finish(r, pre, back)

    def forward_in(j):
        pre = [jnp.dot(T[r, :], W[j, :, :HB], preferred_element_type=F32) for r in halves]
        for r, v in zip(halves, pre):
            a, d = gelu_pair(v)
            act[r, :] = a.astype(BF)
            slope[r, :] = d

    def forward_out(j):
        back = [jnp.dot(C[r, :], W[j, :, HB:], preferred_element_type=F32) for r in halves]
        for r, v in zip(halves, back):
            dpre[r, :] = (v * slope[r, :]).astype(BF)

    def product(r, k):
        q = slice(k * 256, k * 256 + 256)
        return (
            jnp.dot(T[r, q], W[0, q, :HB], preferred_element_type=F32),
            jnp.dot(C[r, q], W[0, q, HB:], preferred_element_type=F32),
        )

    def part(i, k):
        return pl.ds(pl.multiple_of(k * 2 * td + i * BT, BT), BT)

    def early(i, _):
        r = tile(i)
        a, b, d = product(r, 0), product(r, 1), product(r, 3)
        for k in range(2):
            pool[part(i, k), :] = a[k] + b[k] + d[k]
        return 0

    def late(i, _):
        r = tile(i)
        a = product(r, 2)
        finish(r, pool[part(i, 0), :] + a[0], pool[part(i, 1), :] + a[1])
        return 0

    half = td // BT
    half_t = pl.ds(0, td)
    late_t = pl.ds(td, td)

    def tokens_own():
        for k, b in enumerate((T, C)):
            pltpu.make_async_copy(b.at[half_t], b.at[half_t], loc.at[1 + k]).wait()

    def tokens_other():
        for k, b in enumerate((T, C)):
            pltpu.make_async_copy(b.at[late_t], b.at[late_t], tkr.at[k]).wait()

    upper, lower = slice(0, 128), slice(128, 256)

    def rs(u, i):
        to = right if i in (0, 2, 4) else left
        return send(sb.at[u, i], rb.at[u, i], rss.at[0], rsr.at[u, min(i, 2)], to)

    def yc(u, i):
        return send(ys.at[u, i], yr.at[u, i], ycs.at[0], ycr.at[u], across[i])

    def gx(u):
        return pool.at[u * 256 : (u + 1) * 256]

    def gp(u, i):
        at = NU * 256 + u * 256 + i * 128
        return pool.at[at : at + 128]

    def grad(u, ready=lambda: None, sent=lambda: None):
        a, b = ((T, dpre), (C, act))[u % 2]
        dims = (((0,), (0,)), ((), ()))
        far = lax.dot_general(a[:, 512:], b[...], dims, preferred_element_type=F32)
        near = lax.dot_general(a[:, :512], b[...], dims, preferred_element_type=F32)
        for i, v in enumerate((far[:128], far[128:256], near[384:], far[256:384])):
            sb[u, i] = v.astype(BF)
        gx(u)[...] = near[:256]
        gp(u, 0)[...] = near[256:384]
        gp(u, 1)[...] = far[384:]
        ready()
        for i in range(2):
            rs(u, i).start()
        sent()
        for i in range(2, 4):
            rs(u, i).start()

    def whole(ref, sem):
        pltpu.make_async_copy(ref, ref, sem).wait()

    def reduce_one(u):
        for i in range(2):
            rs(u, i).wait_recv()
            sb[u, 4 + i] = (gp(u, i)[...] + rb[u, i].astype(F32)).astype(BF)
            rs(u, 4 + i).start()

    def reduce_two(u):
        whole(rb.at[u, pl.ds(2, 4)], rsr.at[u, 2])
        for r, a, b in ((upper, 3, 4), (lower, 2, 5)):
            gx(u)[r] = gx(u)[r] + rb[u, a].astype(F32) + rb[u, b].astype(F32)
        for i, (yy, cc) in enumerate(((1 - y, c), (1 - y, 1 - c), (y, 1 - c))):
            r = pl.ds(pl.multiple_of(yy * 128 + cc * 64, 64), 64)
            ys[u, i] = gx(u)[r].astype(BF)
            yc(u, i).start()

    def out_copy(buf, ref, k, cols):
        return pltpu.make_async_copy(buf.at[:, cols], ref.at[:, cols], outs.at[k])

    def columns(u, h):
        j, k = u // 2, u % 2
        return pl.ds(pl.multiple_of(k * 2048 + h * 1024 + j * HB, HB), HB)

    def piece(i):
        return slice(i % 2 * 32, i % 2 * 32 + 32), slice(i // 2 * 128, i // 2 * 128 + 128)

    def send_delta(u, o):
        i = lax.rem(me + o, n)
        return send(dl.at[u, i], dr.at[u, me], m1s.at[0], m1r.at[u], (i, s))

    def send_mean(u, o):
        i = lax.rem(me + o, n)
        return send(mr.at[u, me], mr.at[u, me], m2s.at[0], m2r.at[u], (i, s))

    def step(u):
        whole(yr.at[u], ycr.at[u])
        r = pl.ds(pl.multiple_of(y * 128 + c * 64, 64), 64)
        sums = (
            (c, gx(u)[r] + yr[u, 0].astype(F32)),
            (1 - c, yr[u, 1].astype(F32) + yr[u, 2].astype(F32)),
        )
        for h, g in sums:
            cols = columns(u, h)
            first = 0.9 * b1[:, cols] + 0.1 * g
            second = 0.95 * b2[:, cols] + 0.05 * g * g
            root = jnp.sqrt(second * (1.0 / second_correction)) + 1e-08
            update = first * (1.0 / first_correction) / root
            p = mst[:, cols]
            inner = p - 0.001 * (update + 0.1 * p)
            b1[:, cols] = first
            b2[:, cols] = second
            out_copy(b1, o1, 0, cols).start()
            out_copy(b2, o2, 1, cols).start()
            delta = (ba[:, cols] - inner).astype(BF)
            for i in range(4):
                dl[u, 4 * h + i] = delta[piece(i)]
        for o in range(1, 8):
            send_delta(u, o).start()

    def mean(u):
        whole(dr.at[u, pl.ds(0, 7)], m1r.at[u])
        total = dl[u, me].astype(F32)
        for o in range(1, 8):
            total = total + dr[u, lax.rem(me + o, n)].astype(F32)
        mr[u, me] = total / n
        for o in range(1, 8):
            send_mean(u, o).start()

    def outer(u):
        whole(mr.at[u, pl.ds(0, 7)], m2r.at[u])
        for h in range(2):
            cols = columns(u, h)
            start = u % 2 * 2048 + h * 1024 + u // 2 * HB
            for i in range(4):
                r, q_ = piece(i)
                q_ = slice(start + q_.start, start + q_.stop)
                m = mr[u, 4 * h + i]
                momentum = 0.9 * bo[r, q_] + m
                bo[r, q_] = momentum
                ba[r, q_] = ba[r, q_] - 0.7 * (m + 0.9 * momentum)
            out_copy(bo, om, 2, cols).start()
            out_copy(ba, oa, 3, cols).start()

    pass_other(0)
    pass_own(0)
    pass_own(1)
    pass_along_y(1)
    pass_far(0)
    near_x(2)
    tokens_own()
    lax.fori_loop(0, half, early, 0)
    tokens_other()
    lax.fori_loop(half, 2 * half, early, 0)
    pass_far(1)
    near_y(3)
    near_x(3)
    gather_end(0)
    lax.fori_loop(0, 2 * half, late, 0)

    def second():
        pass_own(2)
        pass_along_y(2)

    grad(1, ready=second)
    grad(0, ready=lambda: pass_own(3))

    def at(f, j, k):
        if j >= 0:
            f(2 * j + k)

    p, q = NU - 2, NU - 1
    for j in range(1, NJ):
        last = j == NJ - 1
        gather_end(j)
        if j == 1:
            forward(0, j)
            pass_far(2)
            pass_along_y(3)
            forward(1, j)
        else:
            forward_in(j)
        at(reduce_one, j - 1, 1)
        at(reduce_two, j - 2, 0)
        if last:
            step(1)
            step(0)
        grad(2 * j + 1)
        if j == 1:
            pass_far(3)
        else:
            forward_out(j)
        if j == 2:
            for cp in loads[1:]:
                cp.wait()
        at(reduce_one, j - 1, 0)
        if last:
            step(3)
            grad(2 * j, sent=lambda: reduce_one(q))
        else:
            grad(2 * j)
        at(reduce_two, j - 1, 1)

    step(2)
    mean(1)
    mean(0)
    reduce_one(p)
    reduce_two(p - 2)
    reduce_two(q)
    mean(3)
    reduce_two(p)
    mean(2)
    step(q - 2)
    step(p - 2)
    step(q)
    outer(1)
    outer(0)
    step(p)
    mean(q - 2)
    mean(p - 2)
    outer(3)
    outer(2)
    mean(q)
    mean(p)
    outer(q - 2)
    outer(p - 2)
    outer(q)
    outer(p)

    whole(W.at[:, pl.ds(0, 7 * 64)], s1s.at[0])
    whole(W.at[:, pl.ds(0, 512)], s2s.at[0])
    whole(sb, rss.at[0])
    whole(ys, ycs.at[0])
    whole(dl.at[pl.ds(0, NU - 1)], m1s.at[0])
    whole(mr.at[pl.ds(0, NU - 1)], m2s.at[0])
    for k, b in enumerate((T, C)):
        pltpu.make_async_copy(b.at[half_t], b.at[half_t], tks.at[k]).wait()
    for k, (buf, ref) in enumerate(((b1, o1), (b2, o2), (bo, om), (ba, oa))):
        pltpu.make_async_copy(buf, ref, outs.at[k]).wait()


def write(a, b, c, d, o1, o2, o3, o4, sems):
    pairs = ((a, o1), (b, o2), (c, o3), (d, o4))
    for wait in (False, True):
        for i, (src, dst) in enumerate(pairs):
            copy = pltpu.make_async_copy(src, dst, sems.at[i])
            copy.wait() if wait else copy.start()


def shards(tokens, cotangent, master, moment_one, moment_two, anchor, outer_momentum):
    td, d = tokens.shape
    r, w = master.shape
    vm = pltpu.VMEM
    dma = pltpu.SemaphoreType.DMA
    wide = jax.ShapeDtypeStruct((r, w), F32)
    results = pl.pallas_call(
        kernel,
        out_shape=(wide,) * 4,
        in_specs=[pl.BlockSpec(memory_space=pltpu.HBM)] * 7,
        out_specs=(pl.BlockSpec(memory_space=pl.ANY),) * 4,
        scratch_shapes=[
            vm((2 * td, d), BF), vm((2 * td, d), BF), vm((NJ, d, 2 * HB), BF), vm((NJ, r, 2 * HB), BF),
            vm((r, w), F32), vm((r, w), F32), vm((r, w), F32), vm((r, w), F32), vm((r, w), F32),
            vm((2 * td, HB), BF), vm((2 * td, HB), BF), vm((2 * td, HB), F32), vm((4 * td, HB), F32),
            vm((NU, 6, 128, HB), BF), vm((NU, 6, 128, HB), BF),
            vm((NU, 3, r, HB), BF), vm((NU, 3, r, HB), BF),
            vm((NU, 8, 32, 128), BF), vm((NU, 8, 32, 128), BF), vm((NU, 8, 32, 128), F32),
            dma((7,)), dma((2,)), dma((2,)),
            dma((1,)), dma((NJ, 3)), dma((1,)), dma((NJ, 3)),
            dma((1,)), dma((NU, 3)), dma((1,)), dma((NU,)),
            dma((1,)), dma((NU,)), dma((1,)), dma((NU,)), dma((4,)),
        ],
        compiler_params=pltpu.CompilerParams(
            collective_id=0, has_side_effects=True, vmem_limit_bytes=VMEM_MIB * 1024 * 1024
        ),
        cost_estimate=pl.CostEstimate(
            flops=4 * 2 * td * d * 2048, bytes_accessed=16 << 20, transcendentals=0
        ),
        name="outer_step",
    )(tokens, cotangent, master, moment_one, moment_two, anchor, outer_momentum)
    return pl.pallas_call(
        write,
        out_shape=(wide,) * 4,
        in_specs=[pl.BlockSpec(memory_space=pl.ANY)] * 4,
        out_specs=(pl.BlockSpec(memory_space=pltpu.HBM),) * 4,
        scratch_shapes=[dma((4,))],
        compiler_params=pltpu.CompilerParams(vmem_limit_bytes=1024 * 1024),
        name="write_results",
    )(*results)


def solution(mesh):
    rows = P(("group", "shard"), None)
    own = P("shard", None)
    return jax.shard_map(
        shards,
        mesh=mesh,
        in_specs=(rows, rows, rows, rows, rows, own, own),
        out_specs=(rows, rows, own, own),
        check_vma=False,
    )
```
